32 devices in a mesh: section: 4 (over z), col: 8 (over y, x, core).
Axes of the slice: x: 2, y: 2, z: 4, core: 2. Of those that a mesh axis runs over, the one named last changes fastest.
Arguments:
- tiles: bfloat16 [256, 12, 128, 128], P('col', None, 'section'), may hold values from 0.0099487305 to 1
- offsets: int32 [256, 12], replicated, may hold values from -6 to 6, as said below
- counts: int32 [256], replicated, may hold values from 1 to 12
- ranks: int32 [256, 25, 128, 128], P('col', None, 'section'), may hold values from 0 to 3199, as said below
Outputs:
- pruned: bfloat16 [256, 25, 128, 128], P('col', None, 'section')
The draws below stay inside these ranges and needn't reach their ends.
Inputs may be any that keep to these rules, and one draw needn't show every extreme that they name: Within each panel the 12 offsets are distinct, each from -6 to 6. For every panel j and column c, ranks[j, :, c, :] holds each of 0 .. 3199 once.
All inputs are finite; a program needn't handle non-finite values.
Results may differ from the reference program's by a relative error of at most 0.001.
Values may be sent and summed in bfloat16 or wider, within the bound.
No kernel may reach another device: no remote copies, remote signals or barrier semaphores. Data moves between devices by JAX's collectives and lax.ppermute only.
A program may use at most 128 MiB of HBM per device.

```python
import math
import jax
import jax.numpy as jnp
from jax import lax

TILE = 128
KB = 12
W = 6
TOPK = 256
NB = 256
OB = 25


def draw_offsets(key, part):
    keys = jax.random.split(key, NB)
    perms = jax.vmap(lambda single: jax.random.permutation(single, 2 * W + 1))(keys)
    return (perms[:, :KB] - W).astype(jnp.int32)


def draw_ranks(key, part):
    keys = jax.random.split(key, NB * TILE)
    perms = jax.vmap(lambda single: jax.random.permutation(single, OB * TILE))(keys)
    return perms.reshape(NB, TILE, OB, TILE).transpose(0, 2, 1, 3).astype(jnp.int32)


def place_ends(array, rng, least, largest):
    longest = array.shape.index(max(array.shape))
    spots = []
    for shift in (0, 1):
        where = [jax.random.randint(jax.random.fold_in(rng, axis), (), 0, length) for axis, length in enumerate(array.shape)]
        where[longest] = (where[longest] + shift) % array.shape[longest]
        spots.append(tuple(where))
    return array.at[spots[0]].set(least).at[spots[1]].set(largest)


def levels(stream_key, shape, pieces, least, high):
    def one(position, shards_of):
        heights = jax.random.uniform(jax.random.fold_in(jax.random.fold_in(stream_key, 6), position), (shards_of,), jnp.float32, least / len(pieces), high / len(pieces))
        return jnp.repeat(jnp.exp(heights), shape[position] // shards_of).reshape((-1,) + (1,) * (len(shape) - position - 1))

    factor_of = one(*pieces[0])
    for cut in pieces[1:]:
        factor_of = factor_of * one(*cut)
    return factor_of


def setup_inputs(seed: int = 0) -> dict:
    key_of = jax.random.split(jax.random.key(seed), 5)
    tiles = jnp.clip(jnp.exp(math.log(1.0) - 4.61031033 * jax.random.uniform(key_of[0], (NB, KB, TILE, TILE), jnp.float32) ** levels(key_of[0], (NB, KB, TILE, TILE), ((0, 8), (2, 4)), -0.2, 0.2)), 0.0099487305, 1.0).astype(jnp.bfloat16)
    offsets = draw_offsets(jax.random.fold_in(key_of[4], 71), 0)
    counts = place_ends(jax.random.randint(key_of[2], (NB,), 1, KB + 1), jax.random.fold_in(key_of[2], 1), 1, KB).astype(jnp.int32)
    ranks = draw_ranks(jax.random.fold_in(key_of[4], 71), 0)
    return {"tiles": tiles, "offsets": offsets, "counts": counts, "ranks": ranks}


def reference(tiles, offsets, counts, ranks):
    total = tiles.shape[0]
    slots = tiles.shape[1]
    bands = 4 * W + 1
    padded = jnp.pad(tiles, ((W, W), (0, 0), (0, 0), (0, 0)))
    pad_off = jnp.pad(offsets, ((W, W), (0, 0)))
    pad_cnt = jnp.pad(counts, ((W, W),))
    slot_ids = jnp.arange(slots, dtype=jnp.int32)

    def one_panel(panel):
        own = lax.dynamic_index_in_dim(tiles, panel, 0, False).astype(jnp.float32)
        own_off = lax.dynamic_index_in_dim(offsets, panel, 0, False)
        own_cnt = lax.dynamic_index_in_dim(counts, panel, 0, False)
        where_at = (panel + W + own_off).astype(jnp.int32)
        firsts = padded[where_at].astype(jnp.float32)
        first_off = pad_off[where_at]
        first_cnt = pad_cnt[where_at]
        row_own = panel + own_off
        ok_own = (slot_ids < own_cnt) & (row_own >= 0) & (row_own < total)
        row_first = row_own[:, None] + first_off
        ok_first = (slot_ids[None, :] < first_cnt[:, None]) & (row_first >= 0) & (row_first < total)
        weight = (ok_own[:, None] & ok_first).astype(jnp.float32)
        target = own_off[:, None] + first_off + 2 * W
        place = (jnp.arange(bands, dtype=jnp.int32)[:, None, None] == target[None]).astype(jnp.float32) * weight[None]
        products = jnp.einsum('kcx,klxr->klcr', own, firsts, precision=lax.Precision.HIGHEST)
        expanded = jnp.einsum('okl,klcr->ocr', place, products, precision=lax.Precision.HIGHEST)
        keep = lax.dynamic_index_in_dim(ranks, panel, 0, False) < TOPK
        squared = jnp.where(keep, expanded * expanded, jnp.float32(0.0))
        totals = jnp.sum(squared, axis=(0, 2), keepdims=True)
        return (TOPK * squared / (totals + 1e-6)).astype(jnp.bfloat16)

    return lax.map(one_panel, jnp.arange(total, dtype=jnp.int32))
```

```python
import functools

import jax
import jax.numpy as jnp
import numpy as np
from jax import lax
from jax.experimental import pallas as pl
from jax.experimental.pallas import tpu as pltpu
from jax.sharding import PartitionSpec as P

TOPK = 256
ROW = 16
VMEM_LIMIT = 60 * 1024 * 1024
ANY = pl.BlockSpec(memory_space=pl.ANY)
SMEM = pl.BlockSpec(memory_space=pltpu.SMEM)


def classes(panels, slots, reach):
    full = panels * slots
    step = max(full // 24, 1)
    edge, halo = full // 3, full // 6
    out = [(step * m, edge, halo) for m in (12, 13, 14, 15, 16, 17, 19)]
    out = [c for c in out if c[0] > edge and halo >= reach and edge > halo]
    return out + [(full, 2 * reach * slots, reach * slots)]


def pack_kernel(sizes, reach, cnt_ref, par_ref, tiles_ref, *rest):
    outs = rest[: len(sizes)]
    buf, sems = rest[len(sizes) :]
    panels, slots = tiles_ref.shape[:2]
    first = par_ref[1]

    def put(j, pos):
        buf[pl.ds(pos, slots)] = tiles_ref[j]
        return pos + cnt_ref[first + j]

    pos = lax.fori_loop(panels - reach, panels, put, jnp.int32(0))
    pos = lax.fori_loop(0, reach, put, pos)
    lax.fori_loop(reach, panels - reach, put, pos)
    copies, start = [], 0
    for q, size in enumerate(sizes):
        copies.append(pltpu.make_async_copy(buf.at[pl.ds(start, size)], outs[q], sems.at[q]))
        start += size
    for c in copies:
        c.start()
    for c in copies:
        c.wait()


def pack(tiles, counts, par, sizes, reach):
    panels, slots, cols, rows = tiles.shape
    return pl.pallas_call(
        functools.partial(pack_kernel, sizes, reach),
        out_shape=[jax.ShapeDtypeStruct((s, cols, rows), tiles.dtype) for s in sizes],
        in_specs=[SMEM, SMEM, pl.BlockSpec(memory_space=pltpu.VMEM)],
        out_specs=[ANY] * len(sizes),
        scratch_shapes=[
            pltpu.VMEM((sum(sizes) + slots, cols, rows), tiles.dtype),
            pltpu.SemaphoreType.DMA((len(sizes),)),
        ],
        compiler_params=pltpu.CompilerParams(vmem_limit_bytes=VMEM_LIMIT),
        name="pack",
    )(counts, par, tiles)


def expand_kernel(cfg, tt, oo, par, own_hbm, ranks_hbm, *rest):
    n, sizes, halo, reach, panels = cfg
    per = 2 * n - 1
    chunks = [rest[per * q : per * (q + 1)] for q in range(len(sizes))]
    rest = rest[per * len(sizes) :]
    left, right, out_hbm = rest[:3]
    tall, own, lhs, acc, rk, ob, sem_t, sem_o, sem_rk, sem_ob = rest[3:]
    bands, cols, rows = rk.shape[1:]
    width = 2 * reach + 2
    total = sum(sizes)
    me = par[0]

    load_own = pltpu.make_async_copy(own_hbm, own.at[pl.ds(0, own_hbm.shape[0])], sem_o)
    load_own.start()

    def rank_copy(j, slot):
        return pltpu.make_async_copy(ranks_hbm.at[j], rk.at[slot], sem_rk.at[slot])

    def out_copy(j, slot):
        return pltpu.make_async_copy(ob.at[slot], out_hbm.at[j], sem_ob.at[slot])

    loads = []

    def load(src, start, size, sec, sem, ok):
        c = pltpu.make_async_copy(src, tall.at[pl.ds(start, size), sec], sem_t.at[sem])
        loads.append((c, ok))

    base, sem = 0, 0
    for q, size in enumerate(sizes):
        load(chunks[q][0], base, size, me, sem, None)
        sem += 1
        for h in range(1, n):
            load(chunks[q][h], base, size, jnp.maximum(me - h, 0), sem, me >= h)
            load(chunks[q][n - 1 + h], base, size, jnp.minimum(me + h, n - 1), sem + 1, me + h < n)
            sem += 2
        base += size
    for side, src in enumerate((left, right)):
        for h in range(n):
            load(src.at[h], total + side * halo, halo, lax.rem(me + n - h, n), sem, None)
            sem += 1

    def when(ok, f):
        if ok is None:
            f()
        else:
            pl.when(ok)(f)

    for c, ok in loads:
        when(ok, c.start)
    for s in range(4):
        rank_copy(s, s).start()
    tall[total + 2 * halo] = jnp.zeros(tall.shape[1:], tall.dtype)
    own[own_hbm.shape[0]] = jnp.zeros(own.shape[1:], own.dtype)

    def clear(j, carry):
        acc[j] = jnp.zeros(acc.shape[1:], acc.dtype)
        return carry

    lax.fori_loop(0, panels, clear, 0)
    load_own.wait()
    for c, ok in loads:
        when(ok, c.wait)

    none_t, none_o = total + 2 * halo, own_hbm.shape[0]

    def finish(j):
        slot = lax.rem(j, 4)
        rank_copy(j, slot).wait()

        @pl.when(j >= 4)
        def _():
            out_copy(j - 4, slot).wait()

        part = jnp.zeros((cols, rows), jnp.float32)
        for o in range(bands):
            a = acc[j, o + 1]
            s = jnp.where(rk[slot, o] < TOPK, a * a, 0.0)
            acc[j, o + 1] = s
            part = part + s
        scale = TOPK / (jnp.sum(part, axis=1, keepdims=True) + 1e-6)
        for o in range(bands):
            ob[slot, o] = (acc[j, o + 1] * scale).astype(ob.dtype)
        out_copy(j, slot).start()

        @pl.when(j + 4 < panels)
        def _():
            rank_copy(j + 4, slot).start()

    def pair(p, carry):
        i0 = 2 * p
        where = []
        for jj in range(width):
            jp = i0 + jj
            j = jp - 2 * reach
            where.append(jnp.where((j >= 0) & (j < panels), j, panels))
            one = oo[jp * ROW + 2 * reach - jj] if jj <= 2 * reach else none_o
            two = oo[jp * ROW + 2 * reach + 1 - jj] if jj >= 1 else none_o
            lhs[jj * cols : (jj + 1) * cols, 0:rows] = own[one]
            lhs[jj * cols : (jj + 1) * cols, rows:] = own[two]
        for q in range(width // 2):
            blocks = []
            for e in (2 * q, 2 * q + 1):
                one = tt[i0 * ROW + e] if e <= 2 * reach else none_t
                two = tt[(i0 + 1) * ROW + e - 1] if e >= 1 else none_t
                blocks.append(
                    jnp.concatenate([tall[one].reshape(rows, rows), tall[two].reshape(rows, rows)], axis=0)
                )
            r = jnp.dot(lhs[...], jnp.concatenate(blocks, axis=1), preferred_element_type=jnp.float32)
            for jj in range(width):
                for h in range(2):
                    o = 2 * q + h - jj + 2 * reach + 1
                    if 1 <= o <= bands:
                        acc[where[jj], o] += r[jj * cols : (jj + 1) * cols, h * rows : (h + 1) * rows]

        @pl.when(p >= reach)
        def _():
            finish(i0 - 2 * reach)
            finish(i0 - 2 * reach + 1)

        return carry

    lax.fori_loop(0, (panels + 2 * reach) // 2, pair, 0)
    for s in range(4):
        j = panels - 4 + s
        out_copy(j, j % 4).wait()


def expand(tt, oo, par, own, ranks, chunks, left, right, sizes, halo, reach, n):
    panels, bands, cols, rows = ranks.shape
    flat = [a for chunk in chunks for a in chunk]
    total = sum(sizes)
    n_loads = len(flat) + 2 * n
    return pl.pallas_call(
        functools.partial(expand_kernel, (n, sizes, halo, reach, panels)),
        out_shape=jax.ShapeDtypeStruct(ranks.shape, jnp.bfloat16),
        in_specs=[SMEM, SMEM, SMEM] + [ANY] * (2 + len(flat) + 2),
        out_specs=ANY,
        scratch_shapes=[
            pltpu.VMEM((total + 2 * halo + 1, n, cols, rows), own.dtype),
            pltpu.VMEM((own.shape[0] + 1, cols, rows), own.dtype),
            pltpu.VMEM(((2 * reach + 2) * cols, 2 * rows), own.dtype),
            pltpu.VMEM((panels + 1, bands + 2, cols, rows), jnp.float32),
            pltpu.VMEM((4, bands, cols, rows), jnp.int32),
            pltpu.VMEM((4, bands, cols, rows), jnp.bfloat16),
            pltpu.SemaphoreType.DMA((n_loads,)),
            pltpu.SemaphoreType.DMA,
            pltpu.SemaphoreType.DMA((4,)),
            pltpu.SemaphoreType.DMA((4,)),
        ],
        compiler_params=pltpu.CompilerParams(vmem_limit_bytes=VMEM_LIMIT),
        name="expand",
    )(tt, oo, par, own, ranks, *flat, left, right)


def order_masks(panels, reach):
    window = panels + 2 * reach
    before = np.zeros((window, window), np.int32)
    rank = np.zeros(panels, np.int64)
    order = list(range(panels - reach, panels)) + list(range(panels - reach))
    for position, j in enumerate(order):
        rank[j] = position
    before[reach : reach + panels, reach : reach + panels] = rank[None, :] < rank[:, None]
    for lo in (0, reach + panels):
        before[lo : lo + reach, lo : lo + reach] = np.tri(reach, k=-1, dtype=np.int32)
    return before


def tables(offsets, counts, first, panels, reach, total_panels):
    slots = offsets.shape[1]
    window = panels + 2 * reach
    pad_off = jnp.pad(offsets, ((reach, reach), (0, 0)))
    pad_cnt = jnp.pad(counts, (reach, reach))
    off = lax.dynamic_slice_in_dim(pad_off, first, window, 0)
    cnt = lax.dynamic_slice_in_dim(pad_cnt, first, window, 0)
    row = first - reach + jnp.arange(window, dtype=jnp.int32)[:, None] + off
    k = jnp.arange(slots, dtype=jnp.int32)
    here = (k[None, :] < cnt[:, None]) & (row >= 0) & (row < total_panels)
    hit = here[:, :, None] & (off[:, :, None] + reach == jnp.arange(ROW, dtype=jnp.int32))
    base = jnp.sum(order_masks(panels, reach) * cnt[None, :], axis=1)
    return hit, base


def pick(hit, index, none):
    found = jnp.sum(jnp.where(hit, index[:, :, None] - none, 0), axis=1) + none
    return found.astype(jnp.int32)


def branch(cap, reach, n, ncol, tiles, offsets, counts, ranks):
    size, edge, halo = cap
    panels, slots, cols, rows = tiles.shape
    window = panels + 2 * reach
    sizes = (edge, size - edge)
    col = lax.axis_index("col")
    sec = lax.axis_index("section")
    first = col * panels
    par = jnp.stack([sec, first]).astype(jnp.int32)
    packed = pack(tiles, counts, par, sizes, reach)

    chunks = []
    for q in range(len(sizes)):
        ups, downs = [packed[q]], [packed[q]]
        for h in range(1, n):
            pairs = [(i, i + 1) for i in range(h - 1, n - 1)]
            ups.append(lax.ppermute(ups[-1], "section", pairs))
            downs.append(lax.ppermute(downs[-1], "section", [(n - 1 - i, n - 1 - j) for i, j in pairs]))
        chunks.append([packed[q]] + ups[1:] + downs[1:])

    cnt = lax.dynamic_slice_in_dim(counts, first, panels, 0)
    split = jnp.sum(cnt[panels - reach :])

    def whole(start):
        cut = [lax.dynamic_slice_in_dim(a, start, halo, 0) for a in chunks[0]]
        parts = [cut[0]]
        for h in range(1, n):
            parts.append(jnp.where(sec >= h, cut[h], cut[n - 1 + n - h]))
        return jnp.stack(parts)

    ring = [(i, i + 1) for i in range(ncol - 1)]
    left = lax.ppermute(whole(0), "col", ring)
    right = lax.ppermute(whole(split), "col", [(b, a) for a, b in ring])

    hit, base = tables(offsets, counts, first, panels, reach, offsets.shape[0])
    shift = np.zeros(window, np.int32)
    shift[:reach] = size
    shift[reach + panels :] = size + halo
    k = jnp.arange(slots, dtype=jnp.int32)
    tt = pick(hit, (base + shift)[:, None] + k[None, :], size + 2 * halo)
    mine = jnp.arange(panels, dtype=jnp.int32)[:, None] * slots + k[None, :]
    oo = pick(hit[reach : reach + panels], mine, panels * slots)
    oo = jnp.pad(oo, ((2 * reach, 2 * reach), (0, 0)), constant_values=panels * slots)
    return expand(
        tt.reshape(-1), oo.reshape(-1), par, tiles.reshape(-1, cols, rows), ranks,
        chunks, left, right, sizes, halo, reach, n,
    )


def shards(tiles, offsets, counts, ranks):
    panels, slots = tiles.shape[:2]
    reach = (ranks.shape[1] - 1) // 4
    n = lax.axis_size("section")
    ncol = lax.axis_size("col")
    by_group = counts.reshape(ncol, panels)
    most = jnp.max(jnp.sum(by_group, axis=1))
    most_last = jnp.max(jnp.sum(by_group[:, panels - reach :], axis=1))
    most_first = jnp.max(jnp.sum(by_group[:, :reach], axis=1))
    caps = classes(panels, slots, reach)
    index = jnp.int32(0)
    for size, edge, halo in caps[:-1]:
        fits = (most <= size) & (most_last <= edge - halo) & (most_first <= halo) & (most_last <= halo)
        index = index + (~fits).astype(jnp.int32)
    branches = [functools.partial(branch, c, reach, n, ncol) for c in caps]
    return lax.switch(index, branches, tiles, offsets, counts, ranks)


def solution(mesh):
    placed = (P("col", None, "section", None), P(), P(), P("col", None, "section", None))
    return jax.shard_map(
        shards,
        mesh=mesh,
        in_specs=placed,
        out_specs=P("col", None, "section", None),
        check_vma=False,
    )
```

```python
import functools

import jax
import jax.numpy as jnp
import numpy as np
from jax import lax
from jax.experimental import pallas as pl
from jax.experimental.pallas import tpu as pltpu
from jax.sharding import PartitionSpec as P


TOPK = 256
ROW = 16
VMEM_LIMIT = 32 * 1024 * 1024
ANY = pl.BlockSpec(memory_space=pl.ANY)
SMEM = pl.BlockSpec(memory_space=pltpu.SMEM)
VMEM = pl.BlockSpec(memory_space=pltpu.VMEM)


def classes(panels, slots, reach):
    full = panels * slots
    step = max(full // 24, 1)
    edge, halo = full // 3, full // 6
    out = [(step * m, edge, halo) for m in (14, 15, 16, 17)]
    out = [c for c in out if c[0] > edge and halo >= reach and edge > halo]
    return out + [(full, 2 * reach * slots, reach * slots)]


def params(**kw):
    return pltpu.CompilerParams(vmem_limit_bytes=VMEM_LIMIT, **kw)


def pack_kernel(cfg, cnt_ref, first_ref, tiles_ref, *rest):
    sizes, reach, caps = cfg
    outs = rest[: len(sizes)]
    index_ref, buf, sems = rest[len(sizes) :]
    panels, slots = tiles_ref.shape[:2]
    first = first_ref[0]

    def put(j, pos):
        buf[pl.ds(pos, slots)] = tiles_ref[j]
        return pos + cnt_ref[first + j]

    pos = lax.fori_loop(panels - reach, panels, put, jnp.int32(0))
    pos = lax.fori_loop(0, reach, put, pos)
    lax.fori_loop(reach, panels - reach, put, pos)
    copies, start = [], 0
    for q, size in enumerate(sizes):
        copies.append(pltpu.make_async_copy(buf.at[pl.ds(start, size)], outs[q], sems.at[q]))
        start += size
    for c in copies:
        c.start()

    def group(g, most):
        c = [cnt_ref[g * panels + j] for j in range(panels)]
        lo, hi = sum(c[:reach]), sum(c[panels - reach :])
        return jnp.maximum(most[0], sum(c)), jnp.maximum(most[1], lo), jnp.maximum(most[2], hi)

    zero = jnp.int32(0)
    most, low, high = lax.fori_loop(0, cnt_ref.shape[0] // panels, group, (zero, zero, zero))
    index = jnp.int32(0)
    for size, edge, halo in caps[:-1]:
        fits = (most <= size) & (high <= edge - halo) & (low <= halo) & (high <= halo)
        index = index + jnp.where(fits, 0, 1)
    index_ref[0] = index
    for c in copies:
        c.wait()


def pack(tiles, counts, first, sizes, reach, caps):
    _, slots, cols, rows = tiles.shape
    return pl.pallas_call(
        functools.partial(pack_kernel, (sizes, reach, caps)),
        out_shape=[jax.ShapeDtypeStruct((s, cols, rows), tiles.dtype) for s in sizes]
        + [jax.ShapeDtypeStruct((1,), jnp.int32)],
        in_specs=[SMEM, SMEM, VMEM],
        out_specs=[ANY] * len(sizes) + [SMEM],
        scratch_shapes=[
            pltpu.VMEM((sum(sizes) + slots, cols, rows), tiles.dtype),
            pltpu.SemaphoreType.DMA((len(sizes),)),
        ],
        compiler_params=params(),
        name="pack",
    )(counts, first, tiles)


def edges_kernel(cfg, par, *rest):
    n, sizes, halo = cfg
    per = 2 * n - 1
    chunks = [rest[per * q : per * (q + 1)] for q in range(len(sizes))]
    last, initial, buf, sems = rest[per * len(sizes) :]
    me, split = par[0], par[1]
    base, loads = 0, []
    for q, size in enumerate(sizes):
        for h in range(n):
            dst = buf.at[h, pl.ds(base, size)]
            up = pltpu.make_async_copy(chunks[q][h], dst, sems.at[q * n + h])
            if h == 0:
                loads.append((up, None))
                continue
            down = pltpu.make_async_copy(chunks[q][n - 1 + n - h], dst, sems.at[q * n + h])
            loads += [(up, me >= h), (down, me < h)]
        base += size
    for c, ok in loads:
        when(ok, c.start)
    for c, ok in loads:
        when(ok, c.wait)
    k = len(sizes) * n
    a = pltpu.make_async_copy(buf.at[:, pl.ds(0, halo)], last, sems.at[k])
    b = pltpu.make_async_copy(buf.at[:, pl.ds(split, halo)], initial, sems.at[k + 1])
    a.start()
    b.start()
    a.wait()
    b.wait()


def when(ok, f):
    if ok is None:
        f()
    else:
        pl.when(ok)(f)


def edges(par, chunks, sizes, halo, n):
    flat = [a for chunk in chunks for a in chunk]
    cols, rows = flat[0].shape[1:]
    shape = jax.ShapeDtypeStruct((n, halo, cols, rows), flat[0].dtype)
    return pl.pallas_call(
        functools.partial(edges_kernel, (n, sizes, halo)),
        out_shape=[shape, shape],
        in_specs=[SMEM] + [ANY] * len(flat),
        out_specs=[ANY, ANY],
        scratch_shapes=[
            pltpu.VMEM((n, sum(sizes), cols, rows), flat[0].dtype),
            pltpu.SemaphoreType.DMA((len(sizes) * n + 2,)),
        ],
        compiler_params=params(),
        name="edges",
    )(par, *flat)


def expand_kernel(cfg, tt, oo, par, own_hbm, ranks_hbm, *rest):
    n, which, sizes, halo, reach, panels, opens, writes = cfg
    per = 2 * n - 1
    count = 2 if halo else per * len(sizes)
    given, rest = rest[:count], rest[count:]
    rest = rest[(0 if opens else 1) + (1 if writes == 2 else 0) :]
    acc, rest = rest[0], rest[1:]
    out_hbm = None
    if writes:
        out_hbm, rest = rest[0], rest[1:]
    tall, own, lhs, rk, ob, sem_t, sem_o, sem_rk, sem_ob = rest
    bands, cols, rows = rk.shape[1:]
    width = 2 * reach + 2
    total = 2 * halo if halo else sum(sizes)
    me = par[0]
    lo1, hi1, lo2, hi2, f0, f1 = [par[2 + 6 * which + i] for i in range(6)]
    t0 = which * (tt.shape[0] // 4)

    load_own = pltpu.make_async_copy(own_hbm, own.at[pl.ds(0, own_hbm.shape[0])], sem_o)
    load_own.start()

    def rank_copy(j, slot):
        return pltpu.make_async_copy(ranks_hbm.at[j], rk.at[slot], sem_rk.at[slot])

    def out_copy(j, slot):
        return pltpu.make_async_copy(ob.at[slot], out_hbm.at[j], sem_ob.at[slot])

    loads = []

    def load(src, start, size, sec, ok):
        c = pltpu.make_async_copy(src, tall.at[pl.ds(start, size), sec], sem_t.at[len(loads)])
        loads.append((c, ok))

    if halo:
        for side in range(2):
            for h in range(n):
                load(given[side].at[h], side * halo, halo, lax.rem(me + n - h, n), None)
    base = 0
    for q, size in enumerate(sizes):
        chunk = given[per * q : per * (q + 1)]
        load(chunk[0], base, size, me, None)
        for h in range(1, n):
            load(chunk[h], base, size, jnp.maximum(me - h, 0), me >= h)
            load(chunk[n - 1 + h], base, size, jnp.minimum(me + h, n - 1), me + h < n)
        base += size
    for c, ok in loads:
        when(ok, c.start)
    if writes:
        for s in range(4):
            j = f0 + s
            pl.when(j < f1)(lambda j=j: rank_copy(j, lax.rem(j, 4)).start())
    tall[total] = jnp.zeros(tall.shape[1:], tall.dtype)
    own[own_hbm.shape[0]] = jnp.zeros(own.shape[1:], own.dtype)

    if opens:

        def clear(j, carry):
            acc[j] = jnp.zeros(acc.shape[1:], acc.dtype)
            return carry

        lax.fori_loop(0, panels, clear, 0)
    load_own.wait()
    for c, ok in loads:
        when(ok, c.wait)

    none_t, none_o = total, own_hbm.shape[0]

    def finish(j, carry):
        slot = lax.rem(j, 4)
        rank_copy(j, slot).wait()

        @pl.when(j >= f0 + 4)
        def _():
            out_copy(j - 4, slot).wait()

        part = jnp.zeros((cols, rows), jnp.float32)
        for o in range(bands):
            a = acc[j, o + 1]
            s = jnp.where(rk[slot, o] < TOPK, a * a, 0.0)
            acc[j, o + 1] = s
            part = part + s
        scale = TOPK / (jnp.sum(part, axis=1, keepdims=True) + 1e-6)
        for o in range(bands):
            ob[slot, o] = (acc[j, o + 1] * scale).astype(ob.dtype)
        out_copy(j, slot).start()

        @pl.when(j + 4 < f1)
        def _():
            rank_copy(j + 4, slot).start()

        return carry

    def pair(p, carry):
        i0 = 2 * p
        where = []
        for jj in range(width):
            jp = i0 + jj
            j = jp - 2 * reach
            where.append(jnp.where((j >= 0) & (j < panels), j, panels))
            one = oo[jp * ROW + 2 * reach - jj] if jj <= 2 * reach else none_o
            two = oo[jp * ROW + 2 * reach + 1 - jj] if jj >= 1 else none_o
            lhs[jj * cols : (jj + 1) * cols, 0:rows] = own[one]
            lhs[jj * cols : (jj + 1) * cols, rows:] = own[two]
        for q in range(width // 2):
            blocks = []
            for e in (2 * q, 2 * q + 1):
                one = tt[t0 + i0 * ROW + e] if e <= 2 * reach else none_t
                two = tt[t0 + (i0 + 1) * ROW + e - 1] if e >= 1 else none_t
                blocks.append(
                    jnp.concatenate([tall[one].reshape(rows, rows), tall[two].reshape(rows, rows)], axis=0)
                )
            r = jnp.dot(lhs[...], jnp.concatenate(blocks, axis=1), preferred_element_type=jnp.float32)
            for jj in range(width):
                for h in range(2):
                    o = 2 * q + h - jj + 2 * reach + 1
                    if 1 <= o <= bands:
                        acc[where[jj], o] += r[jj * cols : (jj + 1) * cols, h * rows : (h + 1) * rows]
        return carry

    first = hi1 - lo1

    def step(t, carry):
        return pair(jnp.where(t < first, lo1 + t, lo2 + t - first), carry)

    lax.fori_loop(0, first + hi2 - lo2, step, 0)
    if writes:
        lax.fori_loop(f0, f1, finish, 0)

        def drain(j, carry):
            out_copy(j, lax.rem(j, 4)).wait()
            return carry

        lax.fori_loop(jnp.maximum(f0, f1 - 4), f1, drain, 0)


def expand(which, tt, oo, par, own, ranks, given, sizes, halo, reach, n, acc, out, writes, pairs):
    panels, bands, cols, rows = ranks.shape
    total = 2 * halo if halo else sum(sizes)
    operands = [tt, oo, par, own, ranks] + given
    in_specs = [SMEM, SMEM, SMEM] + [ANY] * (2 + len(given))
    out_shape = [pltpu.VMEM((panels + 1, bands + 2, cols, rows), jnp.float32)]
    out_specs, aliases = [VMEM], {}
    if acc is not None:
        aliases[len(operands)] = 0
        operands.append(acc)
        in_specs.append(VMEM)
    if writes:
        out_shape.append(jax.ShapeDtypeStruct(ranks.shape, jnp.bfloat16))
        out_specs.append(ANY)
        if out is not None:
            aliases[len(operands)] = 1
            operands.append(out)
            in_specs.append(ANY)
    flag = 0 if not writes else (2 if out is not None else 1)
    width = 2 * reach + 2
    flops = 2 * pairs * (width * cols) * (2 * rows) * (width * rows)
    return pl.pallas_call(
        functools.partial(expand_kernel, (n, which, sizes, halo, reach, panels, acc is None, flag)),
        out_shape=out_shape,
        in_specs=in_specs,
        out_specs=out_specs,
        scratch_shapes=[
            pltpu.VMEM((total + 1, n, cols, rows), own.dtype),
            pltpu.VMEM((own.shape[0] + 1, cols, rows), own.dtype),
            pltpu.VMEM((width * cols, 2 * rows), own.dtype),
            pltpu.VMEM((4, bands, cols, rows), jnp.int32),
            pltpu.VMEM((4, bands, cols, rows), jnp.bfloat16),
            pltpu.SemaphoreType.DMA((max(2 * n, len(given)),)),
            pltpu.SemaphoreType.DMA,
            pltpu.SemaphoreType.DMA((4,)),
            pltpu.SemaphoreType.DMA((4,)),
        ],
        input_output_aliases=aliases,
        cost_estimate=pl.CostEstimate(flops=flops, bytes_accessed=total * n * cols * rows * 2, transcendentals=0),
        compiler_params=params(),
    )(*operands)


def order_masks(panels, reach):
    window = panels + 2 * reach
    before = np.zeros((window, window), np.int32)
    rank = np.zeros(panels, np.int64)
    order = list(range(panels - reach, panels)) + list(range(panels - reach))
    for position, j in enumerate(order):
        rank[j] = position
    before[reach : reach + panels, reach : reach + panels] = rank[None, :] < rank[:, None]
    for lo in (0, reach + panels):
        before[lo : lo + reach, lo : lo + reach] = np.tri(reach, k=-1, dtype=np.int32)
    return before


def pick(hit, index):
    return jnp.sum(jnp.where(hit, index[:, :, None] + 1, 0), axis=1) - 1


def tables(cap, cuts, offsets, counts, first, panels, reach):
    size, edge, halo = cap
    total_panels, slots = offsets.shape
    window = panels + 2 * reach
    pad_off = jnp.pad(offsets, ((reach, reach), (0, 0)))
    pad_cnt = jnp.pad(counts, (reach, reach))
    off = lax.dynamic_slice_in_dim(pad_off, first, window, 0)
    cnt = lax.dynamic_slice_in_dim(pad_cnt, first, window, 0)
    row = first - reach + jnp.arange(window, dtype=jnp.int32)[:, None] + off
    k = jnp.arange(slots, dtype=jnp.int32)
    here = (k[None, :] < cnt[:, None]) & (row >= 0) & (row < total_panels)
    hit = here[:, :, None] & (off[:, :, None] + reach == jnp.arange(ROW, dtype=jnp.int32))
    base = jnp.sum(order_masks(panels, reach) * cnt[None, :], axis=1)
    shift = np.zeros(window, np.int32)
    shift[:reach] = size
    shift[reach + panels :] = size + halo
    slot = pick(hit, (base + shift)[:, None] + k[None, :])
    lo = np.array([c[0] for c in cuts], np.int32)[:, None, None]
    hi = np.array([c[1] for c in cuts], np.int32)[:, None, None]
    tt = jnp.where((slot >= lo) & (slot < hi), slot - lo, hi - lo)
    mine = jnp.arange(panels, dtype=jnp.int32)[:, None] * slots + k[None, :]
    oo = pick(hit[reach : reach + panels], mine)
    oo = jnp.pad(oo, ((2 * reach, 2 * reach), (0, 0)), constant_values=-1)
    oo = jnp.where(oo < 0, panels * slots, oo)

    mid = slice(2 * reach, panels)
    start, stop = base[mid], base[mid] + cnt[mid]
    bounds = np.array([edge, cuts[2][1], size], np.int32)
    begun = jnp.sum(start[None, :] < bounds[:, None], axis=1)
    done = jnp.sum(stop[None, :] <= bounds[:, None], axis=1)
    top = 2 * reach
    z = jnp.int32(0)
    half, pairs = reach // 2, (panels + 2 * reach + 1) // 2
    up = (top + begun + 1) // 2
    down = (top + done) // 2
    split = jnp.sum(cnt[panels:reach + panels])
    scalars = [
        lax.axis_index("section"), split,
        z + half, up[0], z + panels // 2, z + (panels + reach + 1) // 2, z, z,
        z, z + (reach + 1) // 2, z + (panels + reach) // 2, z + pairs, z, done[0],
        down[0], up[1], z, z, done[0], done[1],
        down[1], up[2], z, z, done[1], z + panels,
    ]
    return tt.reshape(-1), oo.reshape(-1), jnp.stack([s.astype(jnp.int32) for s in scalars])


def gather(x, n):
    ups, downs = [x], [x]
    for h in range(1, n):
        pairs = [(i, i + 1) for i in range(h - 1, n - 1)]
        ups.append(lax.ppermute(ups[-1], "section", pairs))
        downs.append(lax.ppermute(downs[-1], "section", [(n - 1 - i, n - 1 - j) for i, j in pairs]))
    return [x] + ups[1:] + downs[1:]


def branch(cap, reach, n, ncol, head, tail, tiles, offsets, counts, ranks):
    size, edge, halo = cap
    panels, slots, cols, rows = tiles.shape
    first = lax.axis_index("col") * panels
    extra = edge - 2 * head[0].shape[0]
    two = head[1] if extra == 0 else jnp.concatenate([head[1], tail[:extra]])
    last = min((size - edge) // 2, slots * 4)
    sizes = (head[0].shape[0], two.shape[0])
    more = (size - edge - last, last)
    cuts = [(0, edge), (size, size + 2 * halo), (edge, edge + more[0]), (edge + more[0], size)]
    tt, oo, par = tables(cap, cuts, offsets, counts, first, panels, reach)

    a = [gather(head[0], n), gather(two, n)]
    own = tiles.reshape(-1, cols, rows)
    run = functools.partial(expand, tt=tt, oo=oo, par=par, own=own, ranks=ranks, reach=reach, n=n)
    (acc,) = run(0, given=a[0] + a[1], sizes=sizes, halo=0, acc=None, out=None, writes=False, pairs=11)
    ring = [(i, i + 1) for i in range(ncol - 1)]
    to_next, to_last = edges(par, a, sizes, halo, n)
    left = lax.ppermute(to_next, "col", ring)
    right = lax.ppermute(to_last, "col", [(j, i) for i, j in ring])

    tail, _ = lax.optimization_barrier((tail, (a[0][n - 2], a[0][-2])))
    b = gather(tail[extra : extra + more[0]], n)
    d = gather(tail[extra + more[0] : extra + sum(more)], n)
    acc, out = run(1, given=[left, right], sizes=(), halo=halo, acc=acc, out=None, writes=True, pairs=6)
    acc, out = run(2, given=b, sizes=more[:1], halo=0, acc=acc, out=out, writes=True, pairs=6)
    acc, out = run(3, given=d, sizes=more[1:], halo=0, acc=acc, out=out, writes=True, pairs=5)
    return out


def shards(tiles, offsets, counts, ranks):
    panels, slots = tiles.shape[:2]
    reach = (ranks.shape[1] - 1) // 4
    n = lax.axis_size("section")
    ncol = lax.axis_size("col")
    caps = classes(panels, slots, reach)
    full, edge = panels * slots, caps[0][1]
    sizes = (edge // 2, edge // 2, full - 2 * (edge // 2))
    first = (lax.axis_index("col") * panels).astype(jnp.int32).reshape(1)
    one, two, tail, index = pack(tiles, counts, first, sizes, reach, caps)

    def named(c):
        def run(*args):
            return branch(c, reach, n, ncol, *args)

        return run

    branches = [named(c) for c in caps]
    return lax.switch(index[0], branches, (one, two), tail, tiles, offsets, counts, ranks)


def solution(mesh):
    placed = (P("col", None, "section", None), P(), P(), P("col", None, "section", None))
    return jax.shard_map(
        shards,
        mesh=mesh,
        in_specs=placed,
        out_specs=P("col", None, "section", None),
        check_vma=False,
    )
```
